128 devices in a mesh: replica: 64 (over z, y, x), fsdp: 2 (over core).
Axes of the slice: x: 4, y: 4, z: 4, core: 2. Of those that a mesh axis runs over, the one named last changes fastest.
Arguments:
- block_in: bfloat16 [1, 131072, 896], P(None, ('replica', 'fsdp'))
- grad_out: bfloat16 [131072, 896], P(('replica', 'fsdp'))
- w_up: bfloat16 [1, 896, 4864], P(None, 'fsdp')
- w_lin: bfloat16 [1, 896, 4864], P(None, 'fsdp')
- w_down: bfloat16 [1, 4864, 896], P(None, 'fsdp')
Outputs:
- output 1: float32 [1, 896, 4864], P(None, 'fsdp')
- output 2: float32 [1, 896, 4864], P(None, 'fsdp')
- output 3: float32 [1, 4864, 896], P(None, 'fsdp')
- output 4: bfloat16 [131072, 896], P(('replica', 'fsdp'))
All inputs are finite; a program needn't handle non-finite values.
Results may differ from the reference program's by a relative error of at most 0.001.
Values are sent between devices in bfloat16 or wider.
A program may use at most 1 GiB of HBM per device.

```python
import jax
import jax.numpy as jnp
from jax import lax

D = 896
FF = 4864
LAYERS = 1
TOK_DEV = 1024
REPLICA = 64
FSDP = 2
TOKENS = TOK_DEV * REPLICA * FSDP
NUM_BLOCKS = REPLICA * FSDP
NORM_EPS = 1e-5


def setup_inputs(seed: int = 0) -> dict:
    key_list = jax.random.split(jax.random.key(seed), 5)
    block_in = jax.random.normal(key_list[0], (LAYERS, TOKENS, D), jnp.float32).astype(jnp.bfloat16)
    grad_out = jax.random.normal(key_list[1], (TOKENS, D), jnp.float32).astype(jnp.bfloat16)
    w_up = (jax.random.normal(key_list[2], (LAYERS, D, FF), jnp.float32) * D ** -0.5).astype(jnp.bfloat16)
    w_lin = (jax.random.normal(key_list[3], (LAYERS, D, FF), jnp.float32) * D ** -0.5).astype(jnp.bfloat16)
    w_down = (jax.random.normal(key_list[4], (LAYERS, FF, D), jnp.float32) * (0.5 * FF ** -0.5)).astype(jnp.bfloat16)
    return {'block_in': block_in, 'grad_out': grad_out, 'w_up': w_up, 'w_lin': w_lin, 'w_down': w_down}


def layer_grad(h_in, grad_acc, up_w, lin_w, down_w):
    h_f32 = h_in.astype(jnp.float32)
    inv_rms = lax.rsqrt(jnp.mean(h_f32 * h_f32, axis=-1, keepdims=True) + NORM_EPS)
    normed = h_f32 * inv_rms
    normed_b = normed.astype(jnp.bfloat16)
    pre_up = jnp.dot(normed_b, up_w, preferred_element_type=jnp.float32)
    pre_lin = jnp.dot(normed_b, lin_w, preferred_element_type=jnp.float32)
    up_sig = jax.nn.sigmoid(pre_up)
    up_act = pre_up * up_sig
    act_b = (up_act * pre_lin).astype(jnp.bfloat16)
    grad_b = grad_acc.astype(jnp.bfloat16)
    d_act = jnp.dot(grad_b, down_w.T, preferred_element_type=jnp.float32)
    d_up = (d_act * pre_lin * up_sig * (1.0 + pre_up * (1.0 - up_sig))).astype(jnp.bfloat16)
    d_lin = (d_act * up_act).astype(jnp.bfloat16)
    g_down = jnp.dot(act_b.T, grad_b, preferred_element_type=jnp.float32)
    g_up = jnp.dot(normed_b.T, d_up, preferred_element_type=jnp.float32)
    g_lin = jnp.dot(normed_b.T, d_lin, preferred_element_type=jnp.float32)
    d_norm = jnp.dot(d_up, up_w.T, preferred_element_type=jnp.float32) + jnp.dot(d_lin, lin_w.T, preferred_element_type=jnp.float32)
    d_h = inv_rms * (d_norm - normed * jnp.mean(d_norm * normed, axis=-1, keepdims=True))
    return grad_acc + d_h, g_up, g_lin, g_down


def reference(block_in, grad_out, w_up, w_lin, w_down):
    blocks_in = block_in.reshape(LAYERS, NUM_BLOCKS, TOK_DEV, D).transpose(1, 0, 2, 3)
    blocks_grad = grad_out.reshape(NUM_BLOCKS, TOK_DEV, D)

    def block_step(grad_sums, block_xs):
        h_block, g_block = block_xs

        def layer_step(grad_acc, layer_xs):
            h_layer, up_w, lin_w, down_w = layer_xs
            new_grad, g_up, g_lin, g_down = layer_grad(h_layer, grad_acc, up_w, lin_w, down_w)
            return new_grad, (g_up, g_lin, g_down)

        final_grad, layer_grads = lax.scan(layer_step, g_block.astype(jnp.float32), (h_block, w_up, w_lin, w_down), reverse=True)
        new_sums = tuple(old_part + new_part for old_part, new_part in zip(grad_sums, layer_grads))
        return new_sums, final_grad.astype(jnp.bfloat16)

    zero_sums = (jnp.zeros((LAYERS, D, FF), jnp.float32), jnp.zeros((LAYERS, D, FF), jnp.float32), jnp.zeros((LAYERS, FF, D), jnp.float32))
    grad_sums, grad_blocks = lax.scan(block_step, zero_sums, (blocks_in, blocks_grad))
    return grad_sums[0], grad_sums[1], grad_sums[2], grad_blocks.reshape(TOKENS, D)
```

```python
import jax
import jax.numpy as jnp
from jax import lax
from jax.experimental import pallas as pl
from jax.experimental.pallas import tpu as pltpu
from jax.sharding import PartitionSpec as P

NORM_EPS = 1e-5
MESH = pl.DeviceIdType.MESH
F32 = jnp.float32
BF16 = jnp.bfloat16

D = 896
TOK = 1024
FF = 4864
HALF = FF // 2
SLAB = 128
N_SLAB = HALF // SLAB
CHUNK = 256
N_CHUNK = -(-HALF // CHUNK)
LAST = HALF - (N_CHUNK - 1) * CHUNK
ROWS = D // 2
TILE = 256
BLK = (224, 56, 16)
HALVES = (((0, 112), (112, 112)), ((0, 32), (32, 24)), ((0, 8), (8, 8)))
N_STAGE = 14


def dot(a, b, dims):
    return lax.dot_general(a, b, (dims, ((), ())), preferred_element_type=F32)


def kernel(h_ref, g_ref, w1_ref, w3_ref, w2_ref,
           o1_ref, o3_ref, o2_ref, oh_ref, wx_ref, dnx_ref,
           slab, l3, l3g, ra0, rb0, ra1, rb1, ra2, rb2,
           n_v, nt_v, gb_v, gt_v, dn_v, a_v, du_v, dv_v, w1_v, w3_v, w2_v, tb_v, dnr_v, hr_v, oh_v,
           send_sem, recv_sem, out_sem, xs_sem, xr_sem, w_sem, ws_sem, wr_sem, in_sem, is_sem, ir_sem, fin_sem):
    rep = lax.axis_index("replica")
    core = lax.axis_index("fsdp")
    coord = (lax.rem(rep, 4), lax.rem(lax.div(rep, 4), 4), lax.div(rep, 16))
    stride = (1, 4, 16)
    right = []
    left = []
    for d in range(3):
        right.append((rep + stride[d] * (lax.rem(coord[d] + 1, 4) - coord[d]), core))
        left.append((rep + stride[d] * (lax.rem(coord[d] + 3, 4) - coord[d]), core))
    peer = (rep, 1 - core)
    ra = (ra0, ra1, ra2)
    rb = (rb0, rb1, rb2)

    def rows(level, s, c, block, off, size, gather=False):
        base = block * BLK[level] + off
        if level == 1:
            base = base + coord[c] * BLK[0]
        ref = slab if level < 2 else (l3g if gather else l3)
        return ref.at[s, c, pl.ds(pl.multiple_of(base, 8), size), :]

    def copies(q, s, c):
        par = lax.rem(s, 2)
        if q < 6:
            level, second, gather = q // 2, q % 2, False
        else:
            level, second, gather = 2 - (q - 6) // 2, q % 2, True
        d = (c + level) % 3
        i = coord[d]
        blk = BLK[level]
        (f0, fn), (s0, sn) = HALVES[level]
        if not gather:
            if second == 0:
                b = lax.rem(i + 2, 4)
                pairs = ((rows(level, s, c, b, f0, fn), ra[level].at[par, c, 0, pl.ds(0, fn), :]),
                         (rows(level, s, c, b, s0, sn), ra[level].at[par, c, 1, pl.ds(0, sn), :]))
            else:
                pairs = ((rows(level, s, c, lax.rem(i + 1, 4), 0, blk), rb[level].at[par, c, 0]),
                         (rows(level, s, c, lax.rem(i + 3, 4), 0, blk), rb[level].at[par, c, 1]))
        else:
            if second == 0:
                own = rows(level, s, c, i, 0, blk, True)
                pairs = ((own, own), (own, own))
            else:
                to_right = rows(level, s, c, lax.rem(i + 3, 4), s0, sn, True)
                to_left = rows(level, s, c, lax.rem(i + 1, 4), f0, fn, True)
                pairs = ((to_right, to_right), (to_left, to_left))
        out = []
        for way, (src, dst) in enumerate(pairs):
            out.append(pltpu.make_async_remote_copy(
                src_ref=src, dst_ref=dst,
                send_sem=send_sem.at[par, q, 2 * c + way], recv_sem=recv_sem.at[par, q, 2 * c + way],
                device_id=(right[d], left[d])[way], device_id_type=MESH))
        return out

    def send(q, s):
        for c in range(3):
            for cp in copies(q, s, c):
                cp.start()

    def wait(q, s):
        for c in range(3):
            for cp in copies(q, s, c):
                cp.wait()

    def add_first(level, s):
        par = lax.rem(s, 2)
        (f0, fn), (s0, sn) = HALVES[level]
        for c in range(3):
            i = coord[(c + level) % 3]
            one = rows(level, s, c, lax.rem(i + 1, 4), f0, fn)
            one[...] = one[...] + ra[level][par, c, 0, 0:fn, :]
            two = rows(level, s, c, lax.rem(i + 3, 4), s0, sn)
            two[...] = two[...] + ra[level][par, c, 1, 0:sn, :]

    def add_second(level, s):
        par = lax.rem(s, 2)
        for c in range(3):
            i = coord[(c + level) % 3]
            own = rows(level, s, c, i, 0, BLK[level])
            total = own[...] + rb[level][par, c, 0] + rb[level][par, c, 1]
            if level == 1:
                l3[s, c, 0:56, :] = total
                l3[s, c, 56:64, :] = jnp.zeros((8, SLAB), F32)
            else:
                rows(level, s, c, i, 0, BLK[level], True)[...] = total

    def out_copies(s):
        par = lax.rem(s, 2)
        cols = pl.ds(pl.multiple_of(core * HALF + s * SLAB, 128), SLAB)
        mine = pl.ds(pl.multiple_of(core * ROWS, 8), ROWS)
        theirs = pl.ds(pl.multiple_of((1 - core) * ROWS, 8), ROWS)
        local, remote = [], []
        for c, o_ref in ((0, o1_ref), (1, o3_ref)):
            local.append(pltpu.make_async_copy(slab.at[s, c, mine, :], o_ref.at[:, cols], out_sem.at[par, c]))
            remote.append(pltpu.make_async_remote_copy(
                src_ref=slab.at[s, c, theirs, :], dst_ref=o_ref.at[:, cols],
                send_sem=xs_sem.at[par, c], recv_sem=xr_sem.at[par, c], device_id=peer, device_id_type=MESH))
        local.append(pltpu.make_async_copy(
            tb_v.at[par], o2_ref.at[pl.ds(pl.multiple_of(s * SLAB, 128), SLAB), :], out_sem.at[par, 2]))
        return local, remote

    def stage(j, s):
        if j == 13:
            local, remote = out_copies(s)
            for cp in local + remote:
                cp.wait()
            return
        if j > 0:
            wait(j - 1, s)
        if j in (1, 3, 5):
            add_first(j // 2, s)
        if j in (2, 4, 6):
            add_second(j // 2 - 1, s)
        if j == 8:
            for c in range(3):
                own = rows(1, s, c, coord[(c + 1) % 3], 0, BLK[1])
                own[...] = l3g[s, c, 0:56, :]
        if j < 12:
            send(j, s)
        else:
            tb_v[lax.rem(s, 2)] = slab[s, 2].T
            local, remote = out_copies(s)
            for cp in remote + local:
                cp.start()

    def w_copies(k, size):
        off = pl.multiple_of(k * CHUNK, 128)
        at = pl.multiple_of(core * HALF + k * CHUNK, 128)
        mine = pl.ds(pl.multiple_of(core * ROWS, 16), ROWS)
        theirs = pl.ds(pl.multiple_of((1 - core) * ROWS, 16), ROWS)
        return [
            pltpu.make_async_copy(w1_ref.at[:, pl.ds(at, size)], w1_v.at[mine, pl.ds(0, size)], w_sem.at[0]),
            pltpu.make_async_copy(w3_ref.at[:, pl.ds(at, size)], w3_v.at[mine, pl.ds(0, size)], w_sem.at[1]),
            pltpu.make_async_copy(w2_ref.at[pl.ds(off, size), :], w2_v.at[pl.ds(0, size), :], w_sem.at[2]),
            pltpu.make_async_copy(wx_ref.at[0, :, pl.ds(off, size)], w1_v.at[theirs, pl.ds(0, size)], w_sem.at[3]),
            pltpu.make_async_copy(wx_ref.at[1, :, pl.ds(off, size)], w3_v.at[theirs, pl.ds(0, size)], w_sem.at[4]),
        ]

    def x_copies(k, size):
        off = pl.multiple_of(k * CHUNK, 128)
        at = pl.multiple_of((1 - core) * HALF + k * CHUNK, 128)
        return [pltpu.make_async_remote_copy(
            src_ref=w_ref.at[:, pl.ds(at, size)], dst_ref=wx_ref.at[m, :, pl.ds(off, size)],
            send_sem=ws_sem.at[k, m], recv_sem=wr_sem.at[k, m], device_id=peer, device_id_type=MESH)
            for m, w_ref in ((0, w1_ref), (1, w3_ref))]

    own_tok = pl.ds(pl.multiple_of(core * TOK, TOK), TOK)
    own_h = pltpu.make_async_copy(h_ref, n_v.at[own_tok, :], in_sem.at[0])
    own_g = pltpu.make_async_copy(g_ref, gb_v.at[own_tok, :], in_sem.at[1])
    own_h.start()
    own_g.start()

    barrier = pltpu.get_barrier_semaphore()
    for dev in right + left + [peer]:
        pl.semaphore_signal(barrier, inc=1, device_id=dev, device_id_type=MESH)
    pl.semaphore_wait(barrier, 7)

    peer_h = pltpu.make_async_remote_copy(
        src_ref=h_ref, dst_ref=n_v.at[own_tok, :], send_sem=is_sem.at[0], recv_sem=ir_sem.at[0],
        device_id=peer, device_id_type=MESH)
    peer_g = pltpu.make_async_remote_copy(
        src_ref=g_ref, dst_ref=gb_v.at[own_tok, :], send_sem=is_sem.at[1], recv_sem=ir_sem.at[1],
        device_id=peer, device_id_type=MESH)
    peer_h.start()
    for cp in x_copies(0, CHUNK):
        cp.start()
    peer_g.start()

    def push(k, _):
        for cp in x_copies(k, CHUNK):
            cp.start()
        return 0

    lax.fori_loop(1, N_CHUNK - 1, push, 0)
    for cp in x_copies(N_CHUNK - 1, LAST):
        cp.start()

    def zero(m, _):
        dn_v[pl.ds(pl.multiple_of(m * 64, 64), 64), :] = jnp.zeros((64, D), F32)
        return 0

    lax.fori_loop(0, 2 * TOK // 64, zero, 0)

    def norm(base):
        def body(m, _):
            at = pl.multiple_of(base + m * 128, 128)
            hf = n_v[pl.ds(at, 128), :].astype(F32)
            inv = lax.rsqrt(jnp.mean(hf * hf, axis=-1, keepdims=True) + NORM_EPS)
            nb = (hf * inv).astype(BF16)
            n_v[pl.ds(at, 128), :] = nb
            nt_v[:, pl.ds(at, 128)] = nb.T
            return 0
        lax.fori_loop(0, TOK // 128, body, 0)

    def flip(base):
        def body(m, _):
            at = pl.multiple_of(base + m * 128, 128)
            gt_v[:, pl.ds(at, 128)] = gb_v[pl.ds(at, 128), :].T
            return 0
        lax.fori_loop(0, TOK // 128, body, 0)

    def w_fetch(k):
        @pl.when(k < N_CHUNK - 1)
        def _():
            for cp in x_copies(k, CHUNK):
                cp.wait()
            for cp in w_copies(k, CHUNK):
                cp.start()

        @pl.when(k == N_CHUNK - 1)
        def _():
            for cp in x_copies(k, LAST):
                cp.wait()
            for cp in w_copies(k, LAST):
                cp.start()
            w1_v[:, LAST:] = jnp.zeros((D, CHUNK - LAST), BF16)
            w3_v[:, LAST:] = jnp.zeros((D, CHUNK - LAST), BF16)
            w2_v[LAST:, :] = jnp.zeros((CHUNK - LAST, D), BF16)

    own_h.wait()
    norm(core * TOK)
    own_g.wait()
    flip(core * TOK)
    w_fetch(0)
    peer_h.wait()
    norm((1 - core) * TOK)
    peer_g.wait()
    flip((1 - core) * TOK)

    def phase_a(k):
        @pl.when(k < N_CHUNK - 1)
        def _():
            for cp in w_copies(k, CHUNK):
                cp.wait()

        @pl.when(k == N_CHUNK - 1)
        def _():
            for cp in w_copies(k, LAST):
                cp.wait()

        def body(m, _):
            at = pl.ds(pl.multiple_of(m * TILE, TILE), TILE)
            nb = n_v[at, :]
            pre_up = dot(nb, w1_v[...], ((1,), (0,)))
            pre_lin = dot(nb, w3_v[...], ((1,), (0,)))
            d_act = dot(gb_v[at, :], w2_v[...], ((1,), (1,)))
            sig = jax.nn.sigmoid(pre_up)
            up_act = pre_up * sig
            a_v[at, :] = (up_act * pre_lin).astype(BF16)
            d_up = (d_act * pre_lin * sig * (1.0 + pre_up * (1.0 - sig))).astype(BF16)
            d_lin = (d_act * up_act).astype(BF16)
            du_v[at, :] = d_up
            dv_v[at, :] = d_lin
            dn_v[at, :] += dot(d_up, w1_v[...], ((1,), (1,))) + dot(d_lin, w3_v[...], ((1,), (1,)))
            return 0

        lax.fori_loop(0, 2 * TOK // TILE, body, 0)

        @pl.when(k < N_CHUNK - 1)
        def _():
            w_fetch(k + 1)

    def phase_b(k):
        s0 = 2 * k
        s1 = 2 * k + 1 - lax.div(k, N_CHUNK - 1)

        def body(m, _):
            at = pl.ds(pl.multiple_of(m * 128, 128), 128)
            for c, (lhs, rhs) in enumerate(((nt_v, du_v), (nt_v, dv_v), (gt_v, a_v))):
                out = dot(lhs[at, :], rhs[...], ((1,), (0,)))
                slab[s1, c, at, :] = out[:, SLAB:]
                slab[s0, c, at, :] = out[:, :SLAB]
            return 0

        lax.fori_loop(0, D // 128, body, 0)

    dn_copy = pltpu.make_async_remote_copy(
        src_ref=dn_v.at[pl.ds(pl.multiple_of((1 - core) * TOK, TOK), TOK), :], dst_ref=dnx_ref,
        send_sem=is_sem.at[2], recv_sem=ir_sem.at[2], device_id=peer, device_id_type=MESH)

    def final(m):
        at = pl.ds(pl.multiple_of(m * TILE, TILE), TILE)
        in1 = pltpu.make_async_copy(dnx_ref.at[at, :], dnr_v, fin_sem.at[0])
        in2 = pltpu.make_async_copy(h_ref.at[at, :], hr_v, fin_sem.at[1])
        in1.start()
        in2.start()
        in1.wait()
        in2.wait()
        mine = pl.multiple_of(core * TOK + m * TILE, TILE)

        def body(p, _):
            sub = pl.ds(pl.multiple_of(p * 64, 64), 64)
            here = pl.ds(pl.multiple_of(mine + p * 64, 64), 64)
            hf = hr_v[sub, :].astype(F32)
            inv = lax.rsqrt(jnp.mean(hf * hf, axis=-1, keepdims=True) + NORM_EPS)
            y = hf * inv
            d_norm = dn_v[here, :] + dnr_v[sub, :]
            d_h = inv * (d_norm - y * jnp.mean(d_norm * y, axis=-1, keepdims=True))
            oh_v[sub, :] = (gb_v[here, :].astype(F32) + d_h).astype(BF16)
            return 0

        lax.fori_loop(0, TILE // 64, body, 0)
        out = pltpu.make_async_copy(oh_v, oh_ref.at[at, :], fin_sem.at[2])
        out.start()
        out.wait()

    def step(tt, _):
        k = lax.div(tt, 2)
        odd = lax.rem(tt, 2)

        @pl.when((odd == 0) & (k < N_CHUNK))
        def _():
            phase_a(k)

        @pl.when((odd == 1) & (k < N_CHUNK))
        def _():
            phase_b(k)

        @pl.when(tt == 2 * N_CHUNK - 1)
        def _():
            dn_copy.start()

        @pl.when(tt == 2 * N_CHUNK + 2)
        def _():
            dn_copy.wait()

        @pl.when((tt >= 2 * N_CHUNK + 2) & (tt < 2 * N_CHUNK + 2 + TOK // TILE))
        def _():
            final(tt - (2 * N_CHUNK + 2))

        for j in reversed(range(N_STAGE)):
            s = tt - 1 - j

            @pl.when((s >= 0) & (s < N_SLAB))
            def _(j=j, s=s):
                stage(j, s)

        return 0

    lax.fori_loop(0, N_SLAB + N_STAGE, step, 0)


def solution(mesh):
    tok_spec = P(('replica', 'fsdp'), None)
    act_spec = P(None, ('replica', 'fsdp'), None)
    weight_spec = P(None, 'fsdp', None)

    def local_step(block_in, grad_out, w_up, w_lin, w_down):
        any_spec = pl.BlockSpec(memory_space=pl.ANY)
        dma = pltpu.SemaphoreType.DMA
        o1, o3, o2, oh, _, _ = pl.pallas_call(
            kernel,
            out_shape=(
                jax.ShapeDtypeStruct((ROWS, FF), F32),
                jax.ShapeDtypeStruct((ROWS, FF), F32),
                jax.ShapeDtypeStruct((HALF, D), F32),
                jax.ShapeDtypeStruct((TOK, D), BF16),
                jax.ShapeDtypeStruct((2, ROWS, HALF), BF16),
                jax.ShapeDtypeStruct((TOK, D), F32),
            ),
            in_specs=[any_spec] * 5,
            out_specs=(any_spec,) * 6,
            scratch_shapes=[
                pltpu.VMEM((N_SLAB, 3, D, SLAB), F32),
                pltpu.VMEM((N_SLAB, 3, 64, SLAB), F32),
                pltpu.VMEM((N_SLAB, 3, 64, SLAB), F32),
                pltpu.VMEM((2, 3, 2, 112, SLAB), F32),
                pltpu.VMEM((2, 3, 2, 224, SLAB), F32),
                pltpu.VMEM((2, 3, 2, 32, SLAB), F32),
                pltpu.VMEM((2, 3, 2, 56, SLAB), F32),
                pltpu.VMEM((2, 3, 2, 8, SLAB), F32),
                pltpu.VMEM((2, 3, 2, 16, SLAB), F32),
                pltpu.VMEM((2 * TOK, D), BF16),
                pltpu.VMEM((D, 2 * TOK), BF16),
                pltpu.VMEM((2 * TOK, D), BF16),
                pltpu.VMEM((D, 2 * TOK), BF16),
                pltpu.VMEM((2 * TOK, D), F32),
                pltpu.VMEM((2 * TOK, CHUNK), BF16),
                pltpu.VMEM((2 * TOK, CHUNK), BF16),
                pltpu.VMEM((2 * TOK, CHUNK), BF16),
                pltpu.VMEM((D, CHUNK), BF16),
                pltpu.VMEM((D, CHUNK), BF16),
                pltpu.VMEM((CHUNK, D), BF16),
                pltpu.VMEM((2, SLAB, D), F32),
                pltpu.VMEM((TILE, D), F32),
                pltpu.VMEM((TILE, D), BF16),
                pltpu.VMEM((TILE, D), BF16),
                dma((2, 12, 6)),
                dma((2, 12, 6)),
                dma((2, 3)),
                dma((2, 2)),
                dma((2, 2)),
                dma((5,)),
                dma((N_CHUNK, 2)),
                dma((N_CHUNK, 2)),
                dma((2,)),
                dma((3,)),
                dma((3,)),
                dma((3,)),
            ],
            compiler_params=pltpu.CompilerParams(
                collective_id=0, has_side_effects=True, vmem_limit_bytes=67043328),
        )(block_in[0], grad_out, w_up[0], w_lin[0], w_down[0])
        return o1[None], o3[None], o2[None], oh

    return jax.shard_map(local_step, mesh=mesh, in_specs=(act_spec, tok_spec, weight_spec, weight_spec, weight_spec), out_specs=(weight_spec, weight_spec, weight_spec, tok_spec), check_vma=False)
```

```python
import jax
import jax.numpy as jnp
from jax import lax
from jax.experimental import pallas as pl
from jax.experimental.pallas import tpu as pltpu
from jax.sharding import PartitionSpec as P

NORM_EPS = 1e-5
MESH = pl.DeviceIdType.MESH
F32 = jnp.float32
BF16 = jnp.bfloat16

D = 896
TOK = 1024
FF = 4864
HALF = FF // 2
SLAB = 128
N_SLAB = HALF // SLAB
CHUNK = 256
N_CHUNK = -(-HALF // CHUNK)
LAST = HALF - (N_CHUNK - 1) * CHUNK
ROWS = D // 2
TILE = 128
TILE_1 = 512
TILE_2 = 1024
TILE_B = 128
BLK = (224, 56, 16)
HALVES = (((0, 112), (112, 112)), ((0, 32), (32, 24)), ((0, 8), (8, 8)))
N_STAGE = 14
FIN = 2 * N_CHUNK + 4


def dot(a, b, dims):
    return lax.dot_general(a, b, (dims, ((), ())), preferred_element_type=F32)


def kernel(h_ref, g_ref, w1_ref, w3_ref, w2_ref,
           slab, oh_ref, wx_ref, dnx_ref,
           l3, l3g, ra0, rb0, ra1, rb1, ra2, rb2,
           n_v, nt_v, gb_v, gt_v, dn_v, a_v, du_v, dv_v, w1_v, w3_v, w2_v, xb, dnr_v, hr_v,
           send_sem, recv_sem, xs_sem, xr_sem, w_sem, ws_sem, wr_sem, in_sem, is_sem, ir_sem, fin_sem):
    rep = lax.axis_index("replica")
    core = lax.axis_index("fsdp")
    coord = (lax.rem(rep, 4), lax.rem(lax.div(rep, 4), 4), lax.div(rep, 16))
    stride = (1, 4, 16)
    right = []
    left = []
    for d in range(3):
        right.append((rep + stride[d] * (lax.rem(coord[d] + 1, 4) - coord[d]), core))
        left.append((rep + stride[d] * (lax.rem(coord[d] + 3, 4) - coord[d]), core))
    peer = (rep, 1 - core)
    ra = (ra0, ra1, ra2)
    rb = (rb0, rb1, rb2)

    def rows(level, s, c, block, off, size, gather=False):
        base = block * BLK[level] + off
        if level == 1:
            base = base + coord[c] * BLK[0]
        ref = slab if level < 2 else (l3g if gather else l3)
        if level == 2:
            s = lax.rem(s, 3 if gather else 2)
        return ref.at[s, c, pl.ds(pl.multiple_of(base, 8), size), :]

    def copies(q, s, c):
        par = lax.rem(s, 2)
        if q < 6:
            level, second, gather = q // 2, q % 2, False
        else:
            level, second, gather = 2 - (q - 6) // 2, q % 2, True
        d = (c + level) % 3
        i = coord[d]
        blk = BLK[level]
        (f0, fn), (s0, sn) = HALVES[level]
        if not gather:
            if second == 0:
                b = lax.rem(i + 2, 4)
                pairs = ((rows(level, s, c, b, f0, fn), ra[level].at[par, c, 0, pl.ds(0, fn), :]),
                         (rows(level, s, c, b, s0, sn), ra[level].at[par, c, 1, pl.ds(0, sn), :]))
            else:
                pairs = ((rows(level, s, c, lax.rem(i + 1, 4), 0, blk), rb[level].at[par, c, 0]),
                         (rows(level, s, c, lax.rem(i + 3, 4), 0, blk), rb[level].at[par, c, 1]))
        else:
            if second == 0:
                own = rows(level, s, c, i, 0, blk, True)
                pairs = ((own, own), (own, own))
            else:
                to_right = rows(level, s, c, lax.rem(i + 3, 4), s0, sn, True)
                to_left = rows(level, s, c, lax.rem(i + 1, 4), f0, fn, True)
                pairs = ((to_right, to_right), (to_left, to_left))
        out = []
        for way, (src, dst) in enumerate(pairs):
            out.append(pltpu.make_async_remote_copy(
                src_ref=src, dst_ref=dst,
                send_sem=send_sem.at[par, q, 2 * c + way], recv_sem=recv_sem.at[par, q, 2 * c + way],
                device_id=(right[d], left[d])[way], device_id_type=MESH))
        return out

    def send(q, s):
        for c in range(3):
            for cp in copies(q, s, c):
                cp.start()

    def wait(q, s):
        for c in range(3):
            for cp in copies(q, s, c):
                cp.wait()

    def add_first(level, s):
        par = lax.rem(s, 2)
        (f0, fn), (s0, sn) = HALVES[level]
        for c in range(3):
            i = coord[(c + level) % 3]
            one = rows(level, s, c, lax.rem(i + 1, 4), f0, fn)
            one[...] = one[...] + ra[level][par, c, 0, 0:fn, :]
            two = rows(level, s, c, lax.rem(i + 3, 4), s0, sn)
            two[...] = two[...] + ra[level][par, c, 1, 0:sn, :]

    def add_second(level, s):
        par = lax.rem(s, 2)
        for c in range(3):
            i = coord[(c + level) % 3]
            own = rows(level, s, c, i, 0, BLK[level])
            total = own[...] + rb[level][par, c, 0] + rb[level][par, c, 1]
            if level == 1:
                l3[par, c, 0:56, :] = total
                l3[par, c, 56:64, :] = jnp.zeros((8, SLAB), F32)
            else:
                rows(level, s, c, i, 0, BLK[level], True)[...] = total

    mine_r = pl.ds(pl.multiple_of(core * ROWS, 8), ROWS)
    theirs_r = pl.ds(pl.multiple_of((1 - core) * ROWS, 8), ROWS)

    def swap(s):
        par = lax.rem(s, 2)
        return [pltpu.make_async_remote_copy(
            src_ref=slab.at[s, c, theirs_r, :], dst_ref=xb.at[par, c],
            send_sem=xs_sem.at[par, c], recv_sem=xr_sem.at[par, c], device_id=peer, device_id_type=MESH)
            for c in range(2)]

    def stage(j, s):
        if j == 13:
            for c, cp in enumerate(swap(s)):
                cp.wait()
                slab[s, c, theirs_r, :] = xb[lax.rem(s, 2), c]
            return
        if j > 0:
            wait(j - 1, s)
        if j in (1, 3, 5):
            add_first(j // 2, s)
        if j in (2, 4, 6):
            add_second(j // 2 - 1, s)
        if j == 8:
            for c in range(3):
                own = rows(1, s, c, coord[(c + 1) % 3], 0, BLK[1])
                own[...] = l3g[lax.rem(s, 3), c, 0:56, :]
        if j < 12:
            send(j, s)
        else:
            for cp in swap(s):
                cp.start()
            for i in range(D // SLAB):
                at = slice(i * SLAB, (i + 1) * SLAB)
                slab[s, 2, at, :] = slab[s, 2, at, :].T

    mine_w = pl.ds(pl.multiple_of(core * ROWS, 16), ROWS)
    theirs_w = pl.ds(pl.multiple_of((1 - core) * ROWS, 16), ROWS)

    def w_own(k, size):
        par = lax.rem(k, 2)
        off = pl.multiple_of(k * CHUNK, 128)
        at = pl.multiple_of(core * HALF + k * CHUNK, 128)
        return [
            pltpu.make_async_copy(w1_ref.at[:, pl.ds(at, size)], w1_v.at[par, mine_w, pl.ds(0, size)], w_sem.at[par, 0]),
            pltpu.make_async_copy(w3_ref.at[:, pl.ds(at, size)], w3_v.at[par, mine_w, pl.ds(0, size)], w_sem.at[par, 1]),
            pltpu.make_async_copy(w2_ref.at[pl.ds(off, size), :], w2_v.at[par, pl.ds(0, size), :], w_sem.at[par, 2]),
        ]

    def w_peer(k, size):
        par = lax.rem(k, 2)
        off = pl.multiple_of(k * CHUNK, 128)
        return [
            pltpu.make_async_copy(wx_ref.at[0, :, pl.ds(off, size)], w1_v.at[par, theirs_w, pl.ds(0, size)], w_sem.at[par, 3]),
            pltpu.make_async_copy(wx_ref.at[1, :, pl.ds(off, size)], w3_v.at[par, theirs_w, pl.ds(0, size)], w_sem.at[par, 4]),
        ]

    def x_copies(k, size):
        off = pl.multiple_of(k * CHUNK, 128)
        at = pl.multiple_of((1 - core) * HALF + k * CHUNK, 128)
        return [pltpu.make_async_remote_copy(
            src_ref=w_ref.at[:, pl.ds(at, size)], dst_ref=wx_ref.at[m, :, pl.ds(off, size)],
            send_sem=ws_sem.at[k, m], recv_sem=wr_sem.at[k, m], device_id=peer, device_id_type=MESH)
            for m, w_ref in ((0, w1_ref), (1, w3_ref))]

    first_at = pl.multiple_of((1 - core) * HALF, 128)
    x_first = [pltpu.make_async_remote_copy(
        src_ref=w_ref.at[:, pl.ds(first_at, CHUNK)], dst_ref=w_v.at[0, mine_w, :],
        send_sem=ws_sem.at[0, m], recv_sem=wr_sem.at[0, m], device_id=peer, device_id_type=MESH)
        for m, w_ref, w_v in ((0, w1_ref, w1_v), (1, w3_ref, w3_v))]

    own_tok = pl.ds(pl.multiple_of(core * TOK, TOK), TOK)
    own_h = pltpu.make_async_copy(h_ref, n_v.at[own_tok, :], in_sem.at[0])
    own_g = pltpu.make_async_copy(g_ref, gb_v.at[own_tok, :], in_sem.at[1])
    own_h.start()
    for cp in w_own(0, CHUNK):
        cp.start()
    own_g.start()

    barrier = pltpu.get_barrier_semaphore()
    for dev in right + left + [peer]:
        pl.semaphore_signal(barrier, inc=1, device_id=dev, device_id_type=MESH)
    pl.semaphore_wait(barrier, 7)

    peer_h = pltpu.make_async_remote_copy(
        src_ref=h_ref, dst_ref=n_v.at[own_tok, :], send_sem=is_sem.at[0], recv_sem=ir_sem.at[0],
        device_id=peer, device_id_type=MESH)
    peer_g = pltpu.make_async_remote_copy(
        src_ref=g_ref, dst_ref=gb_v.at[own_tok, :], send_sem=is_sem.at[1], recv_sem=ir_sem.at[1],
        device_id=peer, device_id_type=MESH)
    for cp in x_first:
        cp.start()
    peer_h.start()
    peer_g.start()

    def push(k, _):
        for cp in x_copies(k, CHUNK):
            cp.start()
        return 0

    lax.fori_loop(1, N_CHUNK - 1, push, 0)
    for cp in x_copies(N_CHUNK - 1, LAST):
        cp.start()

    def zero(m, _):
        dn_v[pl.ds(pl.multiple_of(m * 64, 64), 64), :] = jnp.zeros((64, D), F32)
        return 0

    lax.fori_loop(0, 2 * TOK // 64, zero, 0)

    def norm(base):
        def body(m, _):
            at = pl.multiple_of(base + m * 128, 128)
            hf = n_v[pl.ds(at, 128), :].astype(F32)
            inv = lax.rsqrt(jnp.mean(hf * hf, axis=-1, keepdims=True) + NORM_EPS)
            nb = (hf * inv).astype(BF16)
            n_v[pl.ds(at, 128), :] = nb
            nt_v[:, pl.ds(at, 128)] = nb.T
            return 0
        lax.fori_loop(0, TOK // 128, body, 0)

    def flip(base):
        def body(m, _):
            at = pl.multiple_of(base + m * 128, 128)
            gt_v[:, pl.ds(at, 128)] = gb_v[pl.ds(at, 128), :].T
            return 0
        lax.fori_loop(0, TOK // 128, body, 0)

    def w_fetch(k, size):
        for cp in w_own(k, size):
            cp.start()
        for cp in x_copies(k, size):
            cp.wait()
        for cp in w_peer(k, size):
            cp.start()

    def w_wait(k, size):
        for cp in w_own(k, size) + w_peer(k, size):
            cp.wait()

    own_h.wait()
    norm(core * TOK)
    own_g.wait()
    flip(core * TOK)

    def phase_a1(k):
        par = lax.rem(k, 2)

        @pl.when(k == 0)
        def _():
            for cp in w_own(0, CHUNK) + x_first:
                cp.wait()

        @pl.when((k > 0) & (k < N_CHUNK - 1))
        def _():
            w_wait(k, CHUNK)

        @pl.when(k == N_CHUNK - 1)
        def _():
            w_wait(k, LAST)
            w1_v[par, :, LAST:] = jnp.zeros((D, CHUNK - LAST), BF16)
            w3_v[par, :, LAST:] = jnp.zeros((D, CHUNK - LAST), BF16)
            w2_v[par, LAST:, :] = jnp.zeros((CHUNK - LAST, D), BF16)

        def body(m, _):
            @pl.when((k == 0) & (m == TOK // TILE_1))
            def _():
                peer_h.wait()
                norm((1 - core) * TOK)
                peer_g.wait()
                flip((1 - core) * TOK)

            tile = lax.rem(m + core * (TOK // TILE_1), 2 * TOK // TILE_1)
            at = pl.ds(pl.multiple_of(tile * TILE_1, TILE_1), TILE_1)
            nb = n_v[at, :]
            pre_up = dot(nb, w1_v[par], ((1,), (0,)))
            pre_lin = dot(nb, w3_v[par], ((1,), (0,)))
            d_act = dot(gb_v[at, :], w2_v[par], ((1,), (1,)))
            sig = jax.nn.sigmoid(pre_up)
            up_act = pre_up * sig
            a_v[at, :] = (up_act * pre_lin).astype(BF16)
            du_v[at, :] = (d_act * pre_lin * sig * (1.0 + pre_up * (1.0 - sig))).astype(BF16)
            dv_v[at, :] = (d_act * up_act).astype(BF16)
            return 0

        lax.fori_loop(0, 2 * TOK // TILE_1, body, 0)

    def phase_a2(k):
        par = lax.rem(k, 2)

        def body(m, _):
            at = pl.ds(pl.multiple_of(m * TILE_2, TILE_2), TILE_2)
            dn_v[at, :] += dot(du_v[at, :], w1_v[par], ((1,), (1,))) + dot(dv_v[at, :], w3_v[par], ((1,), (1,)))
            return 0

        lax.fori_loop(0, 2 * TOK // TILE_2, body, 0)

    def phase_b(k):
        s0 = 2 * k
        s1 = 2 * k + 1 - lax.div(k, N_CHUNK - 1)

        def body(m, _):
            at = pl.ds(pl.multiple_of(m * TILE_B, 8), TILE_B)
            for c, (lhs, rhs) in enumerate(((nt_v, du_v), (nt_v, dv_v), (gt_v, a_v))):
                out = dot(lhs[at, :], rhs[...], ((1,), (0,)))
                slab[s1, c, at, :] = out[:, SLAB:]
                slab[s0, c, at, :] = out[:, :SLAB]
            return 0

        lax.fori_loop(0, D // TILE_B, body, 0)

    dn_copy = pltpu.make_async_remote_copy(
        src_ref=dn_v.at[pl.ds(pl.multiple_of((1 - core) * TOK, TOK), TOK), :], dst_ref=dnx_ref,
        send_sem=is_sem.at[2], recv_sem=ir_sem.at[2], device_id=peer, device_id_type=MESH)

    def fin_in(m):
        at = pl.ds(pl.multiple_of(m * TILE, TILE), TILE)
        return [pltpu.make_async_copy(dnx_ref.at[at, :], dnr_v, fin_sem.at[0]),
                pltpu.make_async_copy(h_ref.at[at, :], hr_v, fin_sem.at[1])]

    def final(m):
        for cp in fin_in(m):
            cp.wait()

        mine = pl.multiple_of(core * TOK + m * TILE, TILE)

        def body(p, _):
            sub = pl.ds(pl.multiple_of(p * 64, 64), 64)
            here = pl.ds(pl.multiple_of(mine + p * 64, 64), 64)
            hf = hr_v[sub, :].astype(F32)
            inv = lax.rsqrt(jnp.mean(hf * hf, axis=-1, keepdims=True) + NORM_EPS)
            y = hf * inv
            d_norm = dn_v[here, :] + dnr_v[sub, :]
            d_h = inv * (d_norm - y * jnp.mean(d_norm * y, axis=-1, keepdims=True))
            oh_ref[pl.ds(pl.multiple_of(m * TILE + p * 64, 64), 64), :] = (gb_v[here, :].astype(F32) + d_h).astype(BF16)
            return 0

        lax.fori_loop(0, TILE // 64, body, 0)

        @pl.when(m < TOK // TILE - 1)
        def _():
            for cp in fin_in(m + 1):
                cp.start()

    def step(tt, _):
        k = lax.div(tt, 2)
        odd = lax.rem(tt, 2)

        @pl.when((odd == 0) & (k > 0) & (k <= N_CHUNK))
        def _():
            phase_a2(k - 1)

        @pl.when((tt == 1) | ((odd == 0) & (k > 0) & (k < N_CHUNK - 2)))
        def _():
            w_fetch(k + 1, CHUNK)

        @pl.when((odd == 0) & (k == N_CHUNK - 2))
        def _():
            w_fetch(k + 1, LAST)

        @pl.when((odd == 0) & (k < N_CHUNK))
        def _():
            phase_a1(k)

        @pl.when((odd == 1) & (k < N_CHUNK))
        def _():
            phase_b(k)

        @pl.when(tt == 2 * N_CHUNK)
        def _():
            dn_copy.start()

        @pl.when(tt == FIN - 1)
        def _():
            dn_copy.wait()
            for cp in fin_in(0):
                cp.start()

        @pl.when((tt >= FIN) & (tt < FIN + TOK // TILE))
        def _():
            final(tt - FIN)

        for j in reversed(range(N_STAGE)):
            s = tt - 1 - j

            @pl.when((s >= 0) & (s < N_SLAB))
            def _(j=j, s=s):
                stage(j, s)

        return 0

    lax.fori_loop(0, N_SLAB + N_STAGE, step, 0)


def store_kernel(slab, h_v, o1_ref, o3_ref, o2_ref, oh_ref, sem, h_sem):
    core = lax.axis_index("fsdp")

    def copies(s):
        out = []
        for half, who in enumerate((core, 1 - core)):
            part = pl.ds(pl.multiple_of(who * ROWS, 8), ROWS)
            cols = pl.ds(pl.multiple_of(who * HALF + s * SLAB, 128), SLAB)
            for c, o_ref in ((0, o1_ref), (1, o3_ref)):
                out.append(pltpu.make_async_copy(slab.at[s, c, part, :], o_ref.at[:, cols], sem.at[s, 2 * half + c]))
        to = pl.ds(pl.multiple_of(s * SLAB, 128), SLAB)
        for i in range(D // SLAB):
            at = pl.ds(i * SLAB, SLAB)
            out.append(pltpu.make_async_copy(slab.at[s, 2, at, :], o2_ref.at[to, at], sem.at[s, 4 + i]))
        return out

    def start(s, _):
        for cp in copies(s):
            cp.start()
        return 0

    def wait(s, _):
        for cp in copies(s):
            cp.wait()
        return 0

    h_copy = pltpu.make_async_copy(h_v, oh_ref, h_sem.at[0])
    h_copy.start()
    lax.fori_loop(0, N_SLAB, start, 0)
    lax.fori_loop(0, N_SLAB, wait, 0)
    h_copy.wait()


def solution(mesh):
    tok_spec = P(('replica', 'fsdp'), None)
    act_spec = P(None, ('replica', 'fsdp'), None)
    weight_spec = P(None, 'fsdp', None)

    def local_step(block_in, grad_out, w_up, w_lin, w_down):
        any_spec = pl.BlockSpec(memory_space=pl.ANY)
        dma = pltpu.SemaphoreType.DMA
        vmem_spec = pl.BlockSpec(memory_space=pltpu.VMEM)
        sums, oh, _, _ = pl.pallas_call(
            kernel,
            out_shape=(
                pltpu.VMEM((N_SLAB, 3, D, SLAB), F32),
                pltpu.VMEM((TOK, D), BF16),
                jax.ShapeDtypeStruct((2, ROWS, HALF), BF16),
                jax.ShapeDtypeStruct((TOK, D), F32),
            ),
            in_specs=[any_spec] * 5,
            out_specs=(vmem_spec, vmem_spec, any_spec, any_spec),
            scratch_shapes=[
                pltpu.VMEM((2, 3, 64, SLAB), F32),
                pltpu.VMEM((3, 3, 64, SLAB), F32),
                pltpu.VMEM((2, 3, 2, 112, SLAB), F32),
                pltpu.VMEM((2, 3, 2, 224, SLAB), F32),
                pltpu.VMEM((2, 3, 2, 32, SLAB), F32),
                pltpu.VMEM((2, 3, 2, 56, SLAB), F32),
                pltpu.VMEM((2, 3, 2, 8, SLAB), F32),
                pltpu.VMEM((2, 3, 2, 16, SLAB), F32),
                pltpu.VMEM((2 * TOK, D), BF16),
                pltpu.VMEM((D, 2 * TOK), BF16),
                pltpu.VMEM((2 * TOK, D), BF16),
                pltpu.VMEM((D, 2 * TOK), BF16),
                pltpu.VMEM((2 * TOK, D), F32),
                pltpu.VMEM((2 * TOK, CHUNK), BF16),
                pltpu.VMEM((2 * TOK, CHUNK), BF16),
                pltpu.VMEM((2 * TOK, CHUNK), BF16),
                pltpu.VMEM((2, D, CHUNK), BF16),
                pltpu.VMEM((2, D, CHUNK), BF16),
                pltpu.VMEM((2, CHUNK, D), BF16),
                pltpu.VMEM((2, 2, ROWS, SLAB), F32),
                pltpu.VMEM((TILE, D), F32),
                pltpu.VMEM((TILE, D), BF16),
                dma((2, 12, 6)),
                dma((2, 12, 6)),
                dma((2, 2)),
                dma((2, 2)),
                dma((2, 5)),
                dma((N_CHUNK, 2)),
                dma((N_CHUNK, 2)),
                dma((2,)),
                dma((3,)),
                dma((3,)),
                dma((3,)),
            ],
            compiler_params=pltpu.CompilerParams(
                collective_id=0, has_side_effects=True, vmem_limit_bytes=39000000),
        )(block_in[0], grad_out, w_up[0], w_lin[0], w_down[0])
        o1, o3, o2, oh = pl.pallas_call(
            store_kernel,
            out_shape=(
                jax.ShapeDtypeStruct((ROWS, FF), F32),
                jax.ShapeDtypeStruct((ROWS, FF), F32),
                jax.ShapeDtypeStruct((HALF, D), F32),
                jax.ShapeDtypeStruct((TOK, D), BF16),
            ),
            in_specs=[vmem_spec] * 2,
            out_specs=(any_spec,) * 4,
            scratch_shapes=[dma((N_SLAB, 4 + D // SLAB)), dma((1,))],
            compiler_params=pltpu.CompilerParams(has_side_effects=True, vmem_limit_bytes=1048576),
        )(sums, oh)
        return o1[None], o3[None], o2[None], oh

    return jax.shard_map(local_step, mesh=mesh, in_specs=(act_spec, tok_spec, weight_spec, weight_spec, weight_spec), out_specs=(weight_spec, weight_spec, weight_spec, tok_spec), check_vma=False)
```

```python
import jax
import jax.numpy as jnp
from jax import lax
from jax.experimental import pallas as pl
from jax.experimental.pallas import tpu as pltpu
from jax.sharding import PartitionSpec as P

NORM_EPS = 1e-5
MESH = pl.DeviceIdType.MESH
F32 = jnp.float32
BF16 = jnp.bfloat16

D = 896
TOK = 1024
FF = 4864
HALF = FF // 2
SLAB = 128
N_SLAB = HALF // SLAB
CHUNK = 256
N_CHUNK = -(-HALF // CHUNK)
LAST = HALF - (N_CHUNK - 1) * CHUNK
ROWS = D // 2
TILE = 128
TILE_1 = 512
TILE_2 = 512
TILE_B = 128
BLK = (224, 56, 16)
HALVES = (((0, 112), (112, 112)), ((0, 32), (32, 24)), ((0, 8), (8, 8)))
OFFSET = (0, 2, 4, 5, 6, 7, 8, 9, 10, 11, 12, 14, 16, 17)
N_STAGE = len(OFFSET)
SLOTS_A = (4, 2, 2)
SLOTS_B = (3, 2, 2)
A2 = 2 * N_CHUNK + 1
FIN = A2 + N_CHUNK + 2


def dot(a, b, dims):
    return lax.dot_general(a, b, (dims, ((), ())), preferred_element_type=F32)


def kernel(h_ref, g_ref, w1_ref, w3_ref, w2_ref,
           slab, oh_ref, wx_ref, dnx_ref, dux_ref,
           l3, l3g, ra0, rb0, ra1, rb1, ra2, rb2,
           n_v, nt_v, gb_v, gt_v, dn_v, a_v, du_v, dv_v, w1_v, w3_v, w2_v, xb, dnr_v,
           send_sem, recv_sem, xs_sem, xr_sem, w_sem, ws_sem, wr_sem, in_sem, is_sem, ir_sem, fin_sem, du_sem):
    rep = lax.axis_index("replica")
    core = lax.axis_index("fsdp")
    coord = (lax.rem(rep, 4), lax.rem(lax.div(rep, 4), 4), lax.div(rep, 16))
    stride = (1, 4, 16)
    right = []
    left = []
    for d in range(3):
        right.append((rep + stride[d] * (lax.rem(coord[d] + 1, 4) - coord[d]), core))
        left.append((rep + stride[d] * (lax.rem(coord[d] + 3, 4) - coord[d]), core))
    peer = (rep, 1 - core)
    ra = (ra0, ra1, ra2)
    rb = (rb0, rb1, rb2)

    def rows(level, s, c, block, off, size, gather=False):
        base = block * BLK[level] + off
        if level == 1:
            base = base + coord[c] * BLK[0]
        ref = slab if level < 2 else (l3g if gather else l3)
        if level == 2:
            s = lax.rem(s, 3 if gather else 2)
        return ref.at[s, c, pl.ds(pl.multiple_of(base, 8), size), :]

    def copies(q, s, c):
        par = lax.rem(s, 4)
        if q < 6:
            level, second, gather = q // 2, q % 2, False
        else:
            level, second, gather = 2 - (q - 6) // 2, q % 2, True
        d = (c + level) % 3
        i = coord[d]
        blk = BLK[level]
        (f0, fn), (s0, sn) = HALVES[level]
        if not gather:
            if second == 0:
                b = lax.rem(i + 2, 4)
                at = lax.rem(s, SLOTS_A[level])
                pairs = ((rows(level, s, c, b, f0, fn), ra[level].at[at, c, 0, pl.ds(0, fn), :]),
                         (rows(level, s, c, b, s0, sn), ra[level].at[at, c, 1, pl.ds(0, sn), :]))
            else:
                at = lax.rem(s, SLOTS_B[level])
                pairs = ((rows(level, s, c, lax.rem(i + 1, 4), 0, blk), rb[level].at[at, c, 0]),
                         (rows(level, s, c, lax.rem(i + 3, 4), 0, blk), rb[level].at[at, c, 1]))
        else:
            if second == 0:
                own = rows(level, s, c, i, 0, blk, True)
                pairs = ((own, own), (own, own))
            else:
                to_right = rows(level, s, c, lax.rem(i + 3, 4), s0, sn, True)
                to_left = rows(level, s, c, lax.rem(i + 1, 4), f0, fn, True)
                pairs = ((to_right, to_right), (to_left, to_left))
        out = []
        for way, (src, dst) in enumerate(pairs):
            out.append(pltpu.make_async_remote_copy(
                src_ref=src, dst_ref=dst,
                send_sem=send_sem.at[par, q, 2 * c + way], recv_sem=recv_sem.at[par, q, 2 * c + way],
                device_id=(right[d], left[d])[way], device_id_type=MESH))
        return out

    def send(q, s):
        for c in range(3):
            for cp in copies(q, s, c):
                cp.start()

    def wait(q, s):
        for c in range(3):
            for cp in copies(q, s, c):
                cp.wait()

    def add_first(level, s):
        par = lax.rem(s, SLOTS_A[level])
        (f0, fn), (s0, sn) = HALVES[level]
        for c in range(3):
            i = coord[(c + level) % 3]
            one = rows(level, s, c, lax.rem(i + 1, 4), f0, fn)
            one[...] = one[...] + ra[level][par, c, 0, 0:fn, :]
            two = rows(level, s, c, lax.rem(i + 3, 4), s0, sn)
            two[...] = two[...] + ra[level][par, c, 1, 0:sn, :]

    def add_second(level, s):
        at = lax.rem(s, SLOTS_B[level])
        par = lax.rem(s, 2)
        for c in range(3):
            i = coord[(c + level) % 3]
            own = rows(level, s, c, i, 0, BLK[level])
            total = own[...] + rb[level][at, c, 0] + rb[level][at, c, 1]
            if level == 1:
                l3[par, c, 0:56, :] = total
                l3[par, c, 56:64, :] = jnp.zeros((8, SLAB), F32)
            else:
                rows(level, s, c, i, 0, BLK[level], True)[...] = total

    mine_r = pl.ds(pl.multiple_of(core * ROWS, 8), ROWS)
    theirs_r = pl.ds(pl.multiple_of((1 - core) * ROWS, 8), ROWS)

    def swap(s):
        par = lax.rem(s, 2)
        return [pltpu.make_async_remote_copy(
            src_ref=slab.at[s, c, theirs_r, :], dst_ref=xb.at[par, c],
            send_sem=xs_sem.at[par, c], recv_sem=xr_sem.at[par, c], device_id=peer, device_id_type=MESH)
            for c in range(2)]

    def stage(j, s):
        if j == 13:
            for c, cp in enumerate(swap(s)):
                cp.wait()
                slab[s, c, theirs_r, :] = xb[lax.rem(s, 2), c]
            return
        if j > 0:
            wait(j - 1, s)
        if j in (1, 3, 5):
            add_first(j // 2, s)
        if j in (2, 4, 6):
            add_second(j // 2 - 1, s)
        if j == 8:
            for c in range(3):
                own = rows(1, s, c, coord[(c + 1) % 3], 0, BLK[1])
                own[...] = l3g[lax.rem(s, 3), c, 0:56, :]
        if j < 12:
            send(j, s)
        else:
            for cp in swap(s):
                cp.start()
            for i in range(D // SLAB):
                at = slice(i * SLAB, (i + 1) * SLAB)
                slab[s, 2, at, :] = slab[s, 2, at, :].T

    mine_w = pl.ds(pl.multiple_of(core * ROWS, 16), ROWS)
    theirs_w = pl.ds(pl.multiple_of((1 - core) * ROWS, 16), ROWS)

    def w_own(k, size, down=True):
        par = lax.rem(k, 2)
        off = pl.multiple_of(k * CHUNK, 128)
        at = pl.multiple_of(core * HALF + k * CHUNK, 128)
        out = [
            pltpu.make_async_copy(w1_ref.at[:, pl.ds(at, size)], w1_v.at[par, mine_w, pl.ds(0, size)], w_sem.at[par, 0]),
            pltpu.make_async_copy(w3_ref.at[:, pl.ds(at, size)], w3_v.at[par, mine_w, pl.ds(0, size)], w_sem.at[par, 1]),
        ]
        if down:
            out.append(pltpu.make_async_copy(w2_ref.at[pl.ds(off, size), :], w2_v.at[par, pl.ds(0, size), :], w_sem.at[par, 2]))
        return out

    def w_peer(k, size):
        par = lax.rem(k, 2)
        off = pl.multiple_of(k * CHUNK, 128)
        return [
            pltpu.make_async_copy(wx_ref.at[0, :, pl.ds(off, size)], w1_v.at[par, theirs_w, pl.ds(0, size)], w_sem.at[par, 3]),
            pltpu.make_async_copy(wx_ref.at[1, :, pl.ds(off, size)], w3_v.at[par, theirs_w, pl.ds(0, size)], w_sem.at[par, 4]),
        ]

    def x_copies(k, size):
        off = pl.multiple_of(k * CHUNK, 128)
        at = pl.multiple_of((1 - core) * HALF + k * CHUNK, 128)
        return [pltpu.make_async_remote_copy(
            src_ref=w_ref.at[:, pl.ds(at, size)], dst_ref=wx_ref.at[m, :, pl.ds(off, size)],
            send_sem=ws_sem.at[k, m], recv_sem=wr_sem.at[k, m], device_id=peer, device_id_type=MESH)
            for m, w_ref in ((0, w1_ref), (1, w3_ref))]

    first_at = pl.multiple_of((1 - core) * HALF, 128)
    x_first = [pltpu.make_async_remote_copy(
        src_ref=w_ref.at[:, pl.ds(first_at, CHUNK)], dst_ref=w_v.at[0, mine_w, :],
        send_sem=ws_sem.at[N_CHUNK, m], recv_sem=wr_sem.at[N_CHUNK, m], device_id=peer, device_id_type=MESH)
        for m, w_ref, w_v in ((0, w1_ref, w1_v), (1, w3_ref, w3_v))]

    own_tok = pl.ds(pl.multiple_of(core * TOK, TOK), TOK)
    own_h = pltpu.make_async_copy(h_ref, n_v.at[own_tok, :], in_sem.at[0])
    own_g = pltpu.make_async_copy(g_ref, gb_v.at[own_tok, :], in_sem.at[1])
    own_h.start()
    for cp in w_own(0, CHUNK):
        cp.start()
    own_g.start()

    barrier = pltpu.get_barrier_semaphore()
    for dev in right + left + [peer]:
        pl.semaphore_signal(barrier, inc=1, device_id=dev, device_id_type=MESH)
    pl.semaphore_wait(barrier, 7)

    peer_h = pltpu.make_async_remote_copy(
        src_ref=h_ref, dst_ref=n_v.at[own_tok, :], send_sem=is_sem.at[0], recv_sem=ir_sem.at[0],
        device_id=peer, device_id_type=MESH)
    peer_g = pltpu.make_async_remote_copy(
        src_ref=g_ref, dst_ref=gb_v.at[own_tok, :], send_sem=is_sem.at[1], recv_sem=ir_sem.at[1],
        device_id=peer, device_id_type=MESH)
    for cp in x_first:
        cp.start()
    peer_h.start()
    peer_g.start()

    def push(k, _):
        for cp in x_copies(k, CHUNK):
            cp.start()
        return 0

    lax.fori_loop(1, N_CHUNK - 1, push, 0)
    for cp in x_copies(N_CHUNK - 1, LAST) + x_copies(0, CHUNK):
        cp.start()

    def zero(m, _):
        dn_v[pl.ds(pl.multiple_of(m * 64, 64), 64), :] = jnp.zeros((64, D), F32)
        return 0

    lax.fori_loop(0, 2 * TOK // 64, zero, 0)

    def norm(base):
        def body(m, _):
            at = pl.multiple_of(base + m * 128, 128)
            hf = n_v[pl.ds(at, 128), :].astype(F32)
            inv = lax.rsqrt(jnp.mean(hf * hf, axis=-1, keepdims=True) + NORM_EPS)
            nb = (hf * inv).astype(BF16)
            n_v[pl.ds(at, 128), :] = nb
            nt_v[:, pl.ds(at, 128)] = nb.T
            return 0
        lax.fori_loop(0, TOK // 128, body, 0)

    def flip(base):
        def body(m, _):
            at = pl.multiple_of(base + m * 128, 128)
            gt_v[:, pl.ds(at, 128)] = gb_v[pl.ds(at, 128), :].T
            return 0
        lax.fori_loop(0, TOK // 128, body, 0)

    def w_fetch(k, size):
        for cp in w_own(k, size):
            cp.start()
        for cp in x_copies(k, size):
            cp.wait()
        for cp in w_peer(k, size):
            cp.start()

    def w_wait(k, size):
        for cp in w_own(k, size) + w_peer(k, size):
            cp.wait()

    own_h.wait()
    norm(core * TOK)
    own_g.wait()
    flip(core * TOK)

    def phase_a1(k):
        par = lax.rem(k, 2)

        @pl.when(k == 0)
        def _():
            for cp in w_own(0, CHUNK) + x_first:
                cp.wait()

        @pl.when((k > 0) & (k < N_CHUNK - 1))
        def _():
            w_wait(k, CHUNK)

        @pl.when(k == N_CHUNK - 1)
        def _():
            w_wait(k, LAST)
            w1_v[par, :, LAST:] = jnp.zeros((D, CHUNK - LAST), BF16)
            w3_v[par, :, LAST:] = jnp.zeros((D, CHUNK - LAST), BF16)
            w2_v[par, LAST:, :] = jnp.zeros((CHUNK - LAST, D), BF16)

        def body(m, _):
            @pl.when((k == 0) & (m == TOK // TILE_1))
            def _():
                peer_h.wait()
                norm((1 - core) * TOK)
                peer_g.wait()
                flip((1 - core) * TOK)

            tile = lax.rem(m + core * (TOK // TILE_1), 2 * TOK // TILE_1)
            at = pl.ds(pl.multiple_of(tile * TILE_1, TILE_1), TILE_1)
            nb = n_v[at, :]
            pre_up = dot(nb, w1_v[par], ((1,), (0,)))
            pre_lin = dot(nb, w3_v[par], ((1,), (0,)))
            d_act = dot(gb_v[at, :], w2_v[par], ((1,), (1,)))
            sig = jax.nn.sigmoid(pre_up)
            up_act = pre_up * sig
            a_v[at, :] = (up_act * pre_lin).astype(BF16)
            du_v[at, :] = (d_act * pre_lin * sig * (1.0 + pre_up * (1.0 - sig))).astype(BF16)
            dv_v[at, :] = (d_act * up_act).astype(BF16)
            return 0

        lax.fori_loop(0, 2 * TOK // TILE_1, body, 0)

    def du_save(k):
        return [pltpu.make_async_copy(du_v, dux_ref.at[k, 0], du_sem.at[0]),
                pltpu.make_async_copy(dv_v, dux_ref.at[k, 1], du_sem.at[1])]

    def a2_copies(k, size):
        return [pltpu.make_async_copy(dux_ref.at[k, 0], du_v, du_sem.at[0]),
                pltpu.make_async_copy(dux_ref.at[k, 1], dv_v, du_sem.at[1])] + w_own(k, size, False) + w_peer(k, size)

    def phase_a2(k):
        par = lax.rem(k, 2)

        @pl.when(k < N_CHUNK - 1)
        def _():
            for cp in a2_copies(k, CHUNK):
                cp.wait()

        @pl.when(k == N_CHUNK - 1)
        def _():
            for cp in a2_copies(k, LAST):
                cp.wait()

        def body(m, _):
            at = pl.ds(pl.multiple_of(m * TILE_2, TILE_2), TILE_2)
            dn_v[at, :] += dot(du_v[at, :], w1_v[par], ((1,), (1,))) + dot(dv_v[at, :], w3_v[par], ((1,), (1,)))
            return 0

        lax.fori_loop(0, 2 * TOK // TILE_2, body, 0)

    def phase_b(k):
        s0 = 2 * k
        s1 = 2 * k + 1 - lax.div(k, N_CHUNK - 1)

        def body(m, _):
            at = pl.ds(pl.multiple_of(m * TILE_B, 8), TILE_B)
            for c, (lhs, rhs) in enumerate(((nt_v, du_v), (nt_v, dv_v), (gt_v, a_v))):
                out = dot(lhs[at, :], rhs[...], ((1,), (0,)))
                slab[s1, c, at, :] = out[:, SLAB:]
                slab[s0, c, at, :] = out[:, :SLAB]
            return 0

        lax.fori_loop(0, D // TILE_B, body, 0)

    dn_copy = pltpu.make_async_remote_copy(
        src_ref=dn_v.at[pl.ds(pl.multiple_of((1 - core) * TOK, TOK), TOK), :], dst_ref=dnx_ref,
        send_sem=is_sem.at[2], recv_sem=ir_sem.at[2], device_id=peer, device_id_type=MESH)

    def fin_in(m):
        return [pltpu.make_async_copy(
            dnx_ref.at[pl.ds(pl.multiple_of((m + e) * TILE, TILE), TILE), :], dnr_v.at[e], fin_sem.at[e]) for e in range(2)]

    h_again = pltpu.make_async_copy(h_ref, n_v.at[own_tok, :], fin_sem.at[2])

    def final(m):
        for cp in fin_in(m):
            cp.wait()

        mine = pl.multiple_of(core * TOK + m * TILE, TILE)

        def body(p, _):
            sub = pl.ds(pl.multiple_of(lax.rem(p, TILE // 64) * 64, 64), 64)
            here = pl.ds(pl.multiple_of(mine + p * 64, 64), 64)
            hf = n_v[here, :].astype(F32)
            inv = lax.rsqrt(jnp.mean(hf * hf, axis=-1, keepdims=True) + NORM_EPS)
            y = hf * inv
            d_norm = dn_v[here, :] + dnr_v[lax.div(p, TILE // 64), sub, :]
            d_h = inv * (d_norm - y * jnp.mean(d_norm * y, axis=-1, keepdims=True))
            oh_ref[pl.ds(pl.multiple_of(m * TILE + p * 64, 64), 64), :] = (gb_v[here, :].astype(F32) + d_h).astype(BF16)
            return 0

        lax.fori_loop(0, 2 * TILE // 64, body, 0)

        @pl.when(m < TOK // TILE - 2)
        def _():
            for cp in fin_in(m + 2):
                cp.start()

    def step(tt, _):
        k = lax.div(tt, 2)
        odd = lax.rem(tt, 2)

        @pl.when((odd == 0) & (k > 0) & (k <= N_CHUNK))
        def _():
            for cp in du_save(k - 1):
                cp.wait()

        @pl.when((tt == 1) | ((odd == 0) & (k > 0) & (k < N_CHUNK - 2)))
        def _():
            w_fetch(k + 1, CHUNK)

        @pl.when((odd == 0) & (k == N_CHUNK - 2))
        def _():
            w_fetch(k + 1, LAST)

        @pl.when((odd == 0) & (k < N_CHUNK))
        def _():
            phase_a1(k)
            for cp in du_save(k):
                cp.start()

        @pl.when((odd == 1) & (k < N_CHUNK))
        def _():
            phase_b(k)

        @pl.when((tt >= A2) & (tt < A2 + N_CHUNK))
        def _():
            phase_a2(tt - A2)

        @pl.when(tt == A2 - 1)
        def _():
            for cp in x_copies(0, CHUNK):
                cp.wait()

        @pl.when((tt >= A2 - 1) & (tt < A2 + N_CHUNK - 2))
        def _():
            for cp in a2_copies(tt - A2 + 1, CHUNK):
                cp.start()

        @pl.when(tt == A2 + N_CHUNK - 2)
        def _():
            for cp in a2_copies(N_CHUNK - 1, LAST):
                cp.start()

        @pl.when(tt == A2 + N_CHUNK - 1)
        def _():
            dn_copy.start()
            h_again.start()

        @pl.when(tt == FIN - 1)
        def _():
            dn_copy.wait()
            h_again.wait()
            for cp in fin_in(0):
                cp.start()

        @pl.when((tt >= FIN) & (tt < FIN + TOK // TILE // 2))
        def _():
            final(2 * (tt - FIN))

        for j in reversed(range(N_STAGE)):
            s = tt - 1 - OFFSET[j]

            @pl.when((s >= 0) & (s < N_SLAB))
            def _(j=j, s=s):
                stage(j, s)

        return 0

    lax.fori_loop(0, N_SLAB + OFFSET[-1] + 1, step, 0)


def store_kernel(slab, h_v, o1_ref, o3_ref, o2_ref, oh_ref, sem, h_sem):
    core = lax.axis_index("fsdp")

    def copies(s):
        out = []
        for half, who in enumerate((core, 1 - core)):
            part = pl.ds(pl.multiple_of(who * ROWS, 8), ROWS)
            cols = pl.ds(pl.multiple_of(who * HALF + s * SLAB, 128), SLAB)
            for c, o_ref in ((0, o1_ref), (1, o3_ref)):
                out.append(pltpu.make_async_copy(slab.at[s, c, part, :], o_ref.at[:, cols], sem.at[s, 2 * half + c]))
        to = pl.ds(pl.multiple_of(s * SLAB, 128), SLAB)
        for i in range(D // SLAB):
            at = pl.ds(i * SLAB, SLAB)
            out.append(pltpu.make_async_copy(slab.at[s, 2, at, :], o2_ref.at[to, at], sem.at[s, 4 + i]))
        return out

    def start(s, _):
        for cp in copies(s):
            cp.start()
        return 0

    def wait(s, _):
        for cp in copies(s):
            cp.wait()
        return 0

    h_copy = pltpu.make_async_copy(h_v, oh_ref, h_sem.at[0])
    h_copy.start()
    lax.fori_loop(0, N_SLAB, start, 0)
    lax.fori_loop(0, N_SLAB, wait, 0)
    h_copy.wait()


def solution(mesh):
    tok_spec = P(('replica', 'fsdp'), None)
    act_spec = P(None, ('replica', 'fsdp'), None)
    weight_spec = P(None, 'fsdp', None)

    def local_step(block_in, grad_out, w_up, w_lin, w_down):
        any_spec = pl.BlockSpec(memory_space=pl.ANY)
        dma = pltpu.SemaphoreType.DMA
        vmem_spec = pl.BlockSpec(memory_space=pltpu.VMEM)
        sums, oh, _, _, _ = pl.pallas_call(
            kernel,
            out_shape=(
                pltpu.VMEM((N_SLAB, 3, D, SLAB), F32),
                pltpu.VMEM((TOK, D), BF16),
                jax.ShapeDtypeStruct((2, ROWS, HALF), BF16),
                jax.ShapeDtypeStruct((TOK, D), F32),
                jax.ShapeDtypeStruct((N_CHUNK, 2, 2 * TOK, CHUNK), BF16),
            ),
            in_specs=[any_spec] * 5,
            out_specs=(vmem_spec, vmem_spec, any_spec, any_spec, any_spec),
            scratch_shapes=[
                pltpu.VMEM((2, 3, 64, SLAB), F32),
                pltpu.VMEM((3, 3, 64, SLAB), F32),
                pltpu.VMEM((SLOTS_A[0], 3, 2, 112, SLAB), F32),
                pltpu.VMEM((SLOTS_B[0], 3, 2, 224, SLAB), F32),
                pltpu.VMEM((2, 3, 2, 32, SLAB), F32),
                pltpu.VMEM((2, 3, 2, 56, SLAB), F32),
                pltpu.VMEM((2, 3, 2, 8, SLAB), F32),
                pltpu.VMEM((2, 3, 2, 16, SLAB), F32),
                pltpu.VMEM((2 * TOK, D), BF16),
                pltpu.VMEM((D, 2 * TOK), BF16),
                pltpu.VMEM((2 * TOK, D), BF16),
                pltpu.VMEM((D, 2 * TOK), BF16),
                pltpu.VMEM((2 * TOK, D), F32),
                pltpu.VMEM((2 * TOK, CHUNK), BF16),
                pltpu.VMEM((2 * TOK, CHUNK), BF16),
                pltpu.VMEM((2 * TOK, CHUNK), BF16),
                pltpu.VMEM((2, D, CHUNK), BF16),
                pltpu.VMEM((2, D, CHUNK), BF16),
                pltpu.VMEM((2, CHUNK, D), BF16),
                pltpu.VMEM((2, 2, ROWS, SLAB), F32),
                pltpu.VMEM((2, TILE, D), F32),
                dma((4, 12, 6)),
                dma((4, 12, 6)),
                dma((2, 2)),
                dma((2, 2)),
                dma((2, 5)),
                dma((N_CHUNK + 1, 2)),
                dma((N_CHUNK + 1, 2)),
                dma((2,)),
                dma((3,)),
                dma((3,)),
                dma((3,)),
                dma((2,)),
            ],
            compiler_params=pltpu.CompilerParams(
                collective_id=0, has_side_effects=True, vmem_limit_bytes=39000000),
        )(block_in[0], grad_out, w_up[0], w_lin[0], w_down[0])
        o1, o3, o2, oh = pl.pallas_call(
            store_kernel,
            out_shape=(
                jax.ShapeDtypeStruct((ROWS, FF), F32),
                jax.ShapeDtypeStruct((ROWS, FF), F32),
                jax.ShapeDtypeStruct((HALF, D), F32),
                jax.ShapeDtypeStruct((TOK, D), BF16),
            ),
            in_specs=[vmem_spec] * 2,
            out_specs=(any_spec,) * 4,
            scratch_shapes=[dma((N_SLAB, 4 + D // SLAB)), dma((1,))],
            compiler_params=pltpu.CompilerParams(has_side_effects=True, vmem_limit_bytes=1048576),
        )(sums, oh)
        return o1[None], o3[None], o2[None], oh

    return jax.shard_map(local_step, mesh=mesh, in_specs=(act_spec, tok_spec, weight_spec, weight_spec, weight_spec), out_specs=(weight_spec, weight_spec, weight_spec, tok_spec), check_vma=False)
```

```python
import jax
import jax.numpy as jnp
from jax import lax
from jax.experimental import pallas as pl
from jax.experimental.pallas import tpu as pltpu
from jax.sharding import PartitionSpec as P

NORM_EPS = 1e-5
MESH = pl.DeviceIdType.MESH
F32 = jnp.float32
BF16 = jnp.bfloat16

D = 896
TOK = 1024
FF = 4864
HALF = FF // 2
SLAB = 128
N_SLAB = HALF // SLAB
CHUNK = 256
N_CHUNK = -(-HALF // CHUNK)
LAST = HALF - (N_CHUNK - 1) * CHUNK
ROWS = D // 2
TILE = 128
TILE_1 = 512
TILE_2 = 512
TILE_B = 128
BLK = (224, 56, 16)
HALVES = (((0, 112), (112, 112)), ((0, 32), (32, 24)), ((0, 8), (8, 8)))
OFFSET = (0, 2, 4, 5, 6, 7, 8, 9, 10, 11, 12, 14, 16, 17)
ORDER = (9, 8, 7, 6, 5, 4, 3, 2, 13, 12, 11, 10, 1, 0)
SLOTS_A = (4, 2, 2)
SLOTS_B = (3, 2, 2)
A2 = 2 * N_CHUNK
FIN = A2 + N_CHUNK + 1


def dot(a, b, dims):
    return lax.dot_general(a, b, (dims, ((), ())), preferred_element_type=F32)


def kernel(h_ref, g_ref, w1_ref, w3_ref, w2_ref,
           slab, oh_ref, wx_ref, dnx_ref, dux_ref,
           l3, l3g, ra0, rb0, ra1, rb1, ra2, rb2,
           n_v, nt_v, gb_v, gt_v, dn_v, a_v, du_v, dv_v, w1_v, w3_v, w2_v, xb, dnr_v,
           send_sem, recv_sem, xs_sem, xr_sem, w_sem, ws_sem, wr_sem, in_sem, is_sem, ir_sem, fin_sem, du_sem):
    rep = lax.axis_index("replica")
    core = lax.axis_index("fsdp")
    coord = (lax.rem(rep, 4), lax.rem(lax.div(rep, 4), 4), lax.div(rep, 16))
    stride = (1, 4, 16)
    right = []
    left = []
    for d in range(3):
        right.append((rep + stride[d] * (lax.rem(coord[d] + 1, 4) - coord[d]), core))
        left.append((rep + stride[d] * (lax.rem(coord[d] + 3, 4) - coord[d]), core))
    peer = (rep, 1 - core)
    ra = (ra0, ra1, ra2)
    rb = (rb0, rb1, rb2)

    def rows(level, s, c, block, off, size, gather=False):
        base = block * BLK[level] + off
        if level == 1:
            base = base + coord[c] * BLK[0]
        ref = slab if level < 2 else (l3g if gather else l3)
        if level == 2:
            s = lax.rem(s, 3 if gather else 2)
        return ref.at[s, c, pl.ds(pl.multiple_of(base, 8), size), :]

    def copies(q, s, c):
        par = lax.rem(s, 4)
        if q < 6:
            level, second, gather = q // 2, q % 2, False
        else:
            level, second, gather = 2 - (q - 6) // 2, q % 2, True
        d = (c + level) % 3
        i = coord[d]
        blk = BLK[level]
        (f0, fn), (s0, sn) = HALVES[level]
        if not gather:
            if second == 0:
                b = lax.rem(i + 2, 4)
                at = lax.rem(s, SLOTS_A[level])
                pairs = ((rows(level, s, c, b, f0, fn), ra[level].at[at, c, 0, pl.ds(0, fn), :]),
                         (rows(level, s, c, b, s0, sn), ra[level].at[at, c, 1, pl.ds(0, sn), :]))
            else:
                at = lax.rem(s, SLOTS_B[level])
                pairs = ((rows(level, s, c, lax.rem(i + 1, 4), 0, blk), rb[level].at[at, c, 0]),
                         (rows(level, s, c, lax.rem(i + 3, 4), 0, blk), rb[level].at[at, c, 1]))
        else:
            if second == 0:
                own = rows(level, s, c, i, 0, blk, True)
                pairs = ((own, own), (own, own))
            else:
                to_right = rows(level, s, c, lax.rem(i + 3, 4), s0, sn, True)
                to_left = rows(level, s, c, lax.rem(i + 1, 4), f0, fn, True)
                pairs = ((to_right, to_right), (to_left, to_left))
        out = []
        for way, (src, dst) in enumerate(pairs):
            out.append(pltpu.make_async_remote_copy(
                src_ref=src, dst_ref=dst,
                send_sem=send_sem.at[par, q, 2 * c + way], recv_sem=recv_sem.at[par, q, 2 * c + way],
                device_id=(right[d], left[d])[way], device_id_type=MESH))
        return out

    def send(q, s):
        for c in range(3):
            for cp in copies(q, s, c):
                cp.start()

    def wait(q, s):
        for c in range(3):
            for cp in copies(q, s, c):
                cp.wait()

    def add_first(level, s):
        par = lax.rem(s, SLOTS_A[level])
        (f0, fn), (s0, sn) = HALVES[level]
        for c in range(3):
            i = coord[(c + level) % 3]
            one = rows(level, s, c, lax.rem(i + 1, 4), f0, fn)
            one[...] = one[...] + ra[level][par, c, 0, 0:fn, :]
            two = rows(level, s, c, lax.rem(i + 3, 4), s0, sn)
            two[...] = two[...] + ra[level][par, c, 1, 0:sn, :]

    def add_second(level, s):
        at = lax.rem(s, SLOTS_B[level])
        par = lax.rem(s, 2)
        for c in range(3):
            i = coord[(c + level) % 3]
            own = rows(level, s, c, i, 0, BLK[level])
            total = own[...] + rb[level][at, c, 0] + rb[level][at, c, 1]
            if level == 1:
                l3[par, c, 0:56, :] = total
                l3[par, c, 56:64, :] = jnp.zeros((8, SLAB), F32)
            else:
                rows(level, s, c, i, 0, BLK[level], True)[...] = total

    mine_r = pl.ds(pl.multiple_of(core * ROWS, 8), ROWS)
    theirs_r = pl.ds(pl.multiple_of((1 - core) * ROWS, 8), ROWS)

    def swap(s):
        par = lax.rem(s, 2)
        return [pltpu.make_async_remote_copy(
            src_ref=slab.at[s, c, theirs_r, :], dst_ref=xb.at[par, c],
            send_sem=xs_sem.at[par, c], recv_sem=xr_sem.at[par, c], device_id=peer, device_id_type=MESH)
            for c in range(2)]

    def stage(j, s):
        if j == 13:
            for c, cp in enumerate(swap(s)):
                cp.wait()
                slab[s, c, theirs_r, :] = xb[lax.rem(s, 2), c]
            return
        if j > 0:
            wait(j - 1, s)
        if j in (1, 3, 5):
            add_first(j // 2, s)
        if j in (2, 4, 6):
            add_second(j // 2 - 1, s)
        if j == 8:
            for c in range(3):
                own = rows(1, s, c, coord[(c + 1) % 3], 0, BLK[1])
                own[...] = l3g[lax.rem(s, 3), c, 0:56, :]
        if j < 12:
            send(j, s)
        else:
            for cp in swap(s):
                cp.start()
            for i in range(D // SLAB):
                at = slice(i * SLAB, (i + 1) * SLAB)
                slab[s, 2, at, :] = slab[s, 2, at, :].T

    mine_w = pl.ds(pl.multiple_of(core * ROWS, 16), ROWS)
    theirs_w = pl.ds(pl.multiple_of((1 - core) * ROWS, 16), ROWS)

    def w_own(k, size, down=True):
        par = lax.rem(k, 2)
        off = pl.multiple_of(k * CHUNK, 128)
        at = pl.multiple_of(core * HALF + k * CHUNK, 128)
        out = [
            pltpu.make_async_copy(w1_ref.at[:, pl.ds(at, size)], w1_v.at[par, mine_w, pl.ds(0, size)], w_sem.at[par, 0]),
            pltpu.make_async_copy(w3_ref.at[:, pl.ds(at, size)], w3_v.at[par, mine_w, pl.ds(0, size)], w_sem.at[par, 1]),
        ]
        if down:
            out.append(pltpu.make_async_copy(w2_ref.at[pl.ds(off, size), :], w2_v.at[par, pl.ds(0, size), :], w_sem.at[par, 2]))
        return out

    def w_peer(k, size):
        par = lax.rem(k, 2)
        off = pl.multiple_of(k * CHUNK, 128)
        return [
            pltpu.make_async_copy(wx_ref.at[0, :, pl.ds(off, size)], w1_v.at[par, theirs_w, pl.ds(0, size)], w_sem.at[par, 3]),
            pltpu.make_async_copy(wx_ref.at[1, :, pl.ds(off, size)], w3_v.at[par, theirs_w, pl.ds(0, size)], w_sem.at[par, 4]),
        ]

    def x_copies(k, size):
        off = pl.multiple_of(k * CHUNK, 128)
        at = pl.multiple_of((1 - core) * HALF + k * CHUNK, 128)
        return [pltpu.make_async_remote_copy(
            src_ref=w_ref.at[:, pl.ds(at, size)], dst_ref=wx_ref.at[m, :, pl.ds(off, size)],
            send_sem=ws_sem.at[k, m], recv_sem=wr_sem.at[k, m], device_id=peer, device_id_type=MESH)
            for m, w_ref in ((0, w1_ref), (1, w3_ref))]

    first_at = pl.multiple_of((1 - core) * HALF, 128)
    x_first = [pltpu.make_async_remote_copy(
        src_ref=w_ref.at[:, pl.ds(first_at, CHUNK)], dst_ref=w_v.at[0, mine_w, :],
        send_sem=ws_sem.at[N_CHUNK, m], recv_sem=wr_sem.at[N_CHUNK, m], device_id=peer, device_id_type=MESH)
        for m, w_ref, w_v in ((0, w1_ref, w1_v), (1, w3_ref, w3_v))]

    own_tok = pl.ds(pl.multiple_of(core * TOK, TOK), TOK)
    own_h = pltpu.make_async_copy(h_ref, n_v.at[own_tok, :], in_sem.at[0])
    own_g = pltpu.make_async_copy(g_ref, gb_v.at[own_tok, :], in_sem.at[1])
    own_h.start()
    for cp in w_own(0, CHUNK):
        cp.start()
    own_g.start()

    barrier = pltpu.get_barrier_semaphore()
    for dev in right + left + [peer]:
        pl.semaphore_signal(barrier, inc=1, device_id=dev, device_id_type=MESH)
    pl.semaphore_wait(barrier, 7)

    peer_h = pltpu.make_async_remote_copy(
        src_ref=h_ref, dst_ref=n_v.at[own_tok, :], send_sem=is_sem.at[0], recv_sem=ir_sem.at[0],
        device_id=peer, device_id_type=MESH)
    peer_g = pltpu.make_async_remote_copy(
        src_ref=g_ref, dst_ref=gb_v.at[own_tok, :], send_sem=is_sem.at[1], recv_sem=ir_sem.at[1],
        device_id=peer, device_id_type=MESH)
    for cp in x_first:
        cp.start()
    peer_h.start()
    peer_g.start()

    def push(k, _):
        for cp in x_copies(k, CHUNK):
            cp.start()
        return 0

    lax.fori_loop(1, N_CHUNK - 1, push, 0)
    for cp in x_copies(N_CHUNK - 1, LAST) + x_copies(0, CHUNK):
        cp.start()

    def zero(m, _):
        dn_v[pl.ds(pl.multiple_of(m * 64, 64), 64), :] = jnp.zeros((64, D), F32)
        return 0

    def norm(base):
        def body(m, _):
            at = pl.multiple_of(base + m * 128, 128)
            hf = n_v[pl.ds(at, 128), :].astype(F32)
            inv = lax.rsqrt(jnp.mean(hf * hf, axis=-1, keepdims=True) + NORM_EPS)
            nb = (hf * inv).astype(BF16)
            n_v[pl.ds(at, 128), :] = nb
            nt_v[:, pl.ds(at, 128)] = nb.T
            return 0
        lax.fori_loop(0, TOK // 128, body, 0)

    def flip(base):
        def body(m, _):
            at = pl.multiple_of(base + m * 128, 128)
            gt_v[:, pl.ds(at, 128)] = gb_v[pl.ds(at, 128), :].T
            return 0
        lax.fori_loop(0, TOK // 128, body, 0)

    def w_fetch(k, size):
        for cp in w_own(k, size):
            cp.start()
        for cp in x_copies(k, size):
            cp.wait()
        for cp in w_peer(k, size):
            cp.start()

    def w_wait(k, size):
        for cp in w_own(k, size) + w_peer(k, size):
            cp.wait()

    own_h.wait()
    norm(core * TOK)
    own_g.wait()
    flip(core * TOK)

    def phase_a1(k):
        par = lax.rem(k, 2)

        @pl.when(k == 0)
        def _():
            for cp in w_own(0, CHUNK) + x_first:
                cp.wait()

        @pl.when((k > 0) & (k < N_CHUNK - 1))
        def _():
            w_wait(k, CHUNK)

        @pl.when(k == N_CHUNK - 1)
        def _():
            w_wait(k, LAST)
            w1_v[par, :, LAST:] = jnp.zeros((D, CHUNK - LAST), BF16)
            w3_v[par, :, LAST:] = jnp.zeros((D, CHUNK - LAST), BF16)
            w2_v[par, LAST:, :] = jnp.zeros((CHUNK - LAST, D), BF16)

        def body(m, _):
            @pl.when((k == 0) & (m == TOK // TILE_1))
            def _():
                peer_h.wait()
                norm((1 - core) * TOK)
                peer_g.wait()
                flip((1 - core) * TOK)

            tile = lax.rem(m + core * (TOK // TILE_1), 2 * TOK // TILE_1)
            at = pl.ds(pl.multiple_of(tile * TILE_1, TILE_1), TILE_1)
            nb = n_v[at, :]
            pre_up = dot(nb, w1_v[par], ((1,), (0,)))
            pre_lin = dot(nb, w3_v[par], ((1,), (0,)))
            d_act = dot(gb_v[at, :], w2_v[par], ((1,), (1,)))
            sig = jax.nn.sigmoid(pre_up)
            up_act = pre_up * sig
            a_v[at, :] = (up_act * pre_lin).astype(BF16)
            du_v[at, :] = (d_act * pre_lin * sig * (1.0 + pre_up * (1.0 - sig))).astype(BF16)
            dv_v[at, :] = (d_act * up_act).astype(BF16)
            return 0

        lax.fori_loop(0, 2 * TOK // TILE_1, body, 0)

    def du_save(k):
        return [pltpu.make_async_copy(du_v, dux_ref.at[k, 0], du_sem.at[0]),
                pltpu.make_async_copy(dv_v, dux_ref.at[k, 1], du_sem.at[1])]

    def a2_copies(k, size):
        return [pltpu.make_async_copy(dux_ref.at[k, 0], du_v, du_sem.at[0]),
                pltpu.make_async_copy(dux_ref.at[k, 1], dv_v, du_sem.at[1])] + w_own(k, size, False) + w_peer(k, size)

    def phase_a2(k):
        par = lax.rem(k, 2)

        @pl.when(k < N_CHUNK - 1)
        def _():
            for cp in a2_copies(k, CHUNK):
                cp.wait()

        @pl.when(k == N_CHUNK - 1)
        def _():
            for cp in a2_copies(k, LAST):
                cp.wait()

        def body(m, _):
            at = pl.ds(pl.multiple_of(m * TILE_2, TILE_2), TILE_2)
            dn_v[at, :] += dot(du_v[at, :], w1_v[par], ((1,), (1,))) + dot(dv_v[at, :], w3_v[par], ((1,), (1,)))
            return 0

        lax.fori_loop(0, 2 * TOK // TILE_2, body, 0)

    def phase_b(k):
        s0 = 2 * k
        s1 = 2 * k + 1 - lax.div(k, N_CHUNK - 1)

        def body(m, _):
            at = pl.ds(pl.multiple_of(m * TILE_B, 8), TILE_B)
            for c, (lhs, rhs) in enumerate(((nt_v, du_v), (nt_v, dv_v), (gt_v, a_v))):
                out = dot(lhs[at, :], rhs[...], ((1,), (0,)))
                slab[s1, c, at, :] = out[:, SLAB:]
                slab[s0, c, at, :] = out[:, :SLAB]
            return 0

        lax.fori_loop(0, D // TILE_B, body, 0)

    dn_copy = pltpu.make_async_remote_copy(
        src_ref=dn_v.at[pl.ds(pl.multiple_of((1 - core) * TOK, TOK), TOK), :], dst_ref=dnx_ref,
        send_sem=is_sem.at[2], recv_sem=ir_sem.at[2], device_id=peer, device_id_type=MESH)

    def fin_in(m):
        return [pltpu.make_async_copy(
            dnx_ref.at[pl.ds(pl.multiple_of((m + e) * TILE, TILE), TILE), :], dnr_v.at[e], fin_sem.at[e]) for e in range(2)]

    h_again = pltpu.make_async_copy(h_ref, n_v.at[own_tok, :], fin_sem.at[2])

    def final(m):
        for cp in fin_in(m):
            cp.wait()

        mine = pl.multiple_of(core * TOK + m * TILE, TILE)

        def body(p, _):
            sub = pl.ds(pl.multiple_of(lax.rem(p, TILE // 64) * 64, 64), 64)
            here = pl.ds(pl.multiple_of(mine + p * 64, 64), 64)
            hf = n_v[here, :].astype(F32)
            inv = lax.rsqrt(jnp.mean(hf * hf, axis=-1, keepdims=True) + NORM_EPS)
            y = hf * inv
            d_norm = dn_v[here, :] + dnr_v[lax.div(p, TILE // 64), sub, :]
            d_h = inv * (d_norm - y * jnp.mean(d_norm * y, axis=-1, keepdims=True))
            oh_ref[pl.ds(pl.multiple_of(m * TILE + p * 64, 64), 64), :] = (gb_v[here, :].astype(F32) + d_h).astype(BF16)
            return 0

        lax.fori_loop(0, 2 * TILE // 64, body, 0)

        @pl.when(m < TOK // TILE - 2)
        def _():
            for cp in fin_in(m + 2):
                cp.start()

    def step(tt, _):
        k = lax.div(tt, 2)
        odd = lax.rem(tt, 2)

        @pl.when((odd == 0) & (k > 0) & (k < N_CHUNK))
        def _():
            for cp in du_save(k - 1):
                cp.wait()

        @pl.when((tt == 1) | ((odd == 0) & (k > 0) & (k < N_CHUNK - 2)))
        def _():
            w_fetch(k + 1, CHUNK)

        @pl.when((odd == 0) & (k == N_CHUNK - 2))
        def _():
            w_fetch(k + 1, LAST)

        @pl.when((odd == 0) & (k < N_CHUNK))
        def _():
            phase_a1(k)
            for cp in du_save(k):
                cp.start()

        @pl.when((odd == 1) & (k < N_CHUNK))
        def _():
            phase_b(k)

        @pl.when(tt == 2 * N_CHUNK - 1)
        def _():
            for cp in du_save(N_CHUNK - 1):
                cp.wait()

        @pl.when((tt >= A2) & (tt < A2 + N_CHUNK))
        def _():
            phase_a2(tt - A2)

        @pl.when(tt == A2 - 1)
        def _():
            for cp in x_copies(0, CHUNK):
                cp.wait()
            lax.fori_loop(0, 2 * TOK // 64, zero, 0)

        @pl.when((tt >= A2 - 1) & (tt < A2 + N_CHUNK - 2))
        def _():
            for cp in a2_copies(tt - A2 + 1, CHUNK):
                cp.start()

        @pl.when(tt == A2 + N_CHUNK - 2)
        def _():
            for cp in a2_copies(N_CHUNK - 1, LAST):
                cp.start()

        @pl.when(tt == A2 + N_CHUNK - 1)
        def _():
            dn_copy.start()
            h_again.start()

        @pl.when(tt == FIN - 1)
        def _():
            dn_copy.wait()
            h_again.wait()
            for cp in fin_in(0):
                cp.start()

        @pl.when((tt >= FIN) & (tt < FIN + TOK // TILE // 2))
        def _():
            final(2 * (tt - FIN))

        for j in ORDER:
            s = tt - 1 - OFFSET[j]

            @pl.when((s >= 0) & (s < N_SLAB))
            def _(j=j, s=s):
                stage(j, s)

        return 0

    lax.fori_loop(0, max(N_SLAB + OFFSET[-1] + 1, FIN + TOK // TILE // 2), step, 0)


def store_kernel(slab, h_v, o1_ref, o3_ref, o2_ref, oh_ref, sem, h_sem):
    core = lax.axis_index("fsdp")

    def copies(s):
        out = []
        for half, who in enumerate((core, 1 - core)):
            part = pl.ds(pl.multiple_of(who * ROWS, 8), ROWS)
            cols = pl.ds(pl.multiple_of(who * HALF + s * SLAB, 128), SLAB)
            for c, o_ref in ((0, o1_ref), (1, o3_ref)):
                out.append(pltpu.make_async_copy(slab.at[s, c, part, :], o_ref.at[:, cols], sem.at[s, 2 * half + c]))
        to = pl.ds(pl.multiple_of(s * SLAB, 128), SLAB)
        for i in range(D // SLAB):
            at = pl.ds(i * SLAB, SLAB)
            out.append(pltpu.make_async_copy(slab.at[s, 2, at, :], o2_ref.at[to, at], sem.at[s, 4 + i]))
        return out

    def start(s, _):
        for cp in copies(s):
            cp.start()
        return 0

    def wait(s, _):
        for cp in copies(s):
            cp.wait()
        return 0

    h_copy = pltpu.make_async_copy(h_v, oh_ref, h_sem.at[0])
    h_copy.start()
    lax.fori_loop(0, N_SLAB, start, 0)
    lax.fori_loop(0, N_SLAB, wait, 0)
    h_copy.wait()


def solution(mesh):
    tok_spec = P(('replica', 'fsdp'), None)
    act_spec = P(None, ('replica', 'fsdp'), None)
    weight_spec = P(None, 'fsdp', None)

    def local_step(block_in, grad_out, w_up, w_lin, w_down):
        any_spec = pl.BlockSpec(memory_space=pl.ANY)
        dma = pltpu.SemaphoreType.DMA
        vmem_spec = pl.BlockSpec(memory_space=pltpu.VMEM)
        sums, oh, _, _, _ = pl.pallas_call(
            kernel,
            out_shape=(
                pltpu.VMEM((N_SLAB, 3, D, SLAB), F32),
                pltpu.VMEM((TOK, D), BF16),
                jax.ShapeDtypeStruct((2, ROWS, HALF), BF16),
                jax.ShapeDtypeStruct((TOK, D), F32),
                jax.ShapeDtypeStruct((N_CHUNK, 2, 2 * TOK, CHUNK), BF16),
            ),
            in_specs=[any_spec] * 5,
            out_specs=(vmem_spec, vmem_spec, any_spec, any_spec, any_spec),
            scratch_shapes=[
                pltpu.VMEM((2, 3, 64, SLAB), F32),
                pltpu.VMEM((3, 3, 64, SLAB), F32),
                pltpu.VMEM((SLOTS_A[0], 3, 2, 112, SLAB), F32),
                pltpu.VMEM((SLOTS_B[0], 3, 2, 224, SLAB), F32),
                pltpu.VMEM((2, 3, 2, 32, SLAB), F32),
                pltpu.VMEM((2, 3, 2, 56, SLAB), F32),
                pltpu.VMEM((2, 3, 2, 8, SLAB), F32),
                pltpu.VMEM((2, 3, 2, 16, SLAB), F32),
                pltpu.VMEM((2 * TOK, D), BF16),
                pltpu.VMEM((D, 2 * TOK), BF16),
                pltpu.VMEM((2 * TOK, D), BF16),
                pltpu.VMEM((D, 2 * TOK), BF16),
                pltpu.VMEM((2 * TOK, D), F32),
                pltpu.VMEM((2 * TOK, CHUNK), BF16),
                pltpu.VMEM((2 * TOK, CHUNK), BF16),
                pltpu.VMEM((2 * TOK, CHUNK), BF16),
                pltpu.VMEM((2, D, CHUNK), BF16),
                pltpu.VMEM((2, D, CHUNK), BF16),
                pltpu.VMEM((2, CHUNK, D), BF16),
                pltpu.VMEM((2, 2, ROWS, SLAB), F32),
                pltpu.VMEM((2, TILE, D), F32),
                dma((4, 12, 6)),
                dma((4, 12, 6)),
                dma((2, 2)),
                dma((2, 2)),
                dma((2, 5)),
                dma((N_CHUNK + 1, 2)),
                dma((N_CHUNK + 1, 2)),
                dma((2,)),
                dma((3,)),
                dma((3,)),
                dma((3,)),
                dma((2,)),
            ],
            compiler_params=pltpu.CompilerParams(
                collective_id=0, has_side_effects=True, vmem_limit_bytes=39000000),
        )(block_in[0], grad_out, w_up[0], w_lin[0], w_down[0])
        o1, o3, o2, oh = pl.pallas_call(
            store_kernel,
            out_shape=(
                jax.ShapeDtypeStruct((ROWS, FF), F32),
                jax.ShapeDtypeStruct((ROWS, FF), F32),
                jax.ShapeDtypeStruct((HALF, D), F32),
                jax.ShapeDtypeStruct((TOK, D), BF16),
            ),
            in_specs=[vmem_spec] * 2,
            out_specs=(any_spec,) * 4,
            scratch_shapes=[dma((N_SLAB, 4 + D // SLAB)), dma((1,))],
            compiler_params=pltpu.CompilerParams(has_side_effects=True, vmem_limit_bytes=1048576),
        )(sums, oh)
        return o1[None], o3[None], o2[None], oh

    return jax.shard_map(local_step, mesh=mesh, in_specs=(act_spec, tok_spec, weight_spec, weight_spec, weight_spec), out_specs=(weight_spec, weight_spec, weight_spec, tok_spec), check_vma=False)
```
